32 devices in a mesh: blk: 16 (over z, y, x), sub: 2 (over core).
Axes of the slice: x: 2, y: 2, z: 4, core: 2. Of those that a mesh axis runs over, the one named last changes fastest.
Arguments:
- normal_wind: float32 [32, 55, 768], P(('blk', 'sub')), may hold values from -6 to 6
- density: float32 [32, 55, 256], P(('blk', 'sub')), may hold values from 0.5 to 1.5
- theta_field: float32 [32, 55, 256], P(('blk', 'sub')), may hold values from -6 to 6
- cell_edges: int32 [32, 6, 256], P(('blk', 'sub')), may hold values from 0 to 1663, as said below
- edge_cells: int32 [32, 2, 1664], P(('blk', 'sub')), may hold values from 0 to 703, as said below
- edges_on_edge: int32 [32, 10, 768], P(('blk', 'sub')), may hold values from 0 to 1663, as said below
- send_cells: int32 [32, 7, 64], P(('blk', 'sub')), may hold values from 0 to 255
- send_edges: int32 [32, 7, 128], P(('blk', 'sub')), may hold values from 0 to 767
- cell_weight: float32 [32, 6, 256], P(('blk', 'sub')), may hold values from -4 to 4
- eoe_weight: float32 [32, 10, 768], P(('blk', 'sub')), may hold values from -2 to 2
- vert_coupling: float32 [32, 54, 256], P(('blk', 'sub')), may hold values from 0.05 to 4
Outputs:
- density_tend: float32 [32, 55, 256], P(('blk', 'sub'))
- theta_new: float32 [32, 55, 256], P(('blk', 'sub'))
- tangential_wind: float32 [32, 55, 768], P(('blk', 'sub'))
The draws below stay inside these ranges and needn't reach their ends.
Inputs may be any that keep to these rules, and one draw needn't show every extreme that they name: `cell_edges`: positions in the block's extended edge list: owned edges, then 128 received edges for each slot in order. `edge_cells`: positions in the block's extended cell list: owned cells, then 64 received cells for each slot in order. `edges_on_edge`: positions in the block's extended edge list.
All inputs are finite; a program needn't handle non-finite values.
Results may differ from the reference program's by a relative error of at most 0.0003.
Values sent between devices are 32-bit elements; how exact they have to be, the bound alone decides.
No kernel may reach another device: no remote copies, remote signals or barrier semaphores. Data moves between devices by JAX's collectives and lax.ppermute only.
A program may use at most 64 MiB of HBM per device.

```python
import math
import jax
import jax.numpy as jnp
from jax import lax

LEVELS = 55
CELLS_DEV = 256
EDGES_DEV = 768
HALO_CELLS = 64
HALO_EDGES = 128
SLOTS = 7
CELL_SIDES = 6
EDGE_NEIGHBOURS = 10
BLOCKS = 32
N_BLK = 16
N_SUB = 2


def live_counts(key, salt_value, capacity):
    count_key, full_key = jax.random.split(jax.random.fold_in(key, salt_value))
    counts = jax.random.randint(count_key, (BLOCKS, SLOTS), max(capacity // 4, 1), capacity + 1)
    full_slot = jax.random.randint(full_key, (BLOCKS, 1), 0, SLOTS)
    slot_ids = jnp.arange(SLOTS, dtype=jnp.int32)[None, :]
    return jnp.where(slot_ids == full_slot, capacity, counts)


def table_draw(key, salt_value, table_shape, owned, capacity, counts):
    region_key, owned_key, slot_key, entry_key = jax.random.split(jax.random.fold_in(key, salt_value), 4)
    region = jax.random.randint(region_key, table_shape, 0, 4)
    owned_pick = jax.random.randint(owned_key, table_shape, 0, owned)
    slot_pick = jax.random.randint(slot_key, table_shape, 0, SLOTS)
    slot_live = jnp.take_along_axis(counts[:, None, :], slot_pick.reshape(BLOCKS, 1, -1), axis=2).reshape(table_shape)
    entry_pick = jax.random.randint(entry_key, table_shape, 0, slot_live)
    return jnp.where(region < 3, owned_pick, owned + slot_pick * capacity + entry_pick).astype(jnp.int32)


def draw_cell_edges(key, part):
    return table_draw(key, 11, (BLOCKS, CELL_SIDES, CELLS_DEV), EDGES_DEV, HALO_EDGES, live_counts(key, 21, HALO_EDGES))


def draw_edge_cells(key, part):
    return table_draw(key, 12, (BLOCKS, 2, EDGES_DEV + SLOTS * HALO_EDGES), CELLS_DEV, HALO_CELLS, live_counts(key, 22, HALO_CELLS))


def draw_edges_on_edge(key, part):
    return table_draw(key, 13, (BLOCKS, EDGE_NEIGHBOURS, EDGES_DEV), EDGES_DEV, HALO_EDGES, live_counts(key, 21, HALO_EDGES))


def touch_ends(values, stream_key, smallest, top_value):
    spot = [jax.random.randint(jax.random.fold_in(stream_key, axis), (), 0, length) for axis, length in enumerate(values.shape)]
    main_axis = values.shape.index(max(values.shape))
    beside = spot[:main_axis] + [(spot[main_axis] + 1) % values.shape[main_axis]] + spot[main_axis + 1:]
    return values.at[tuple(spot)].set(smallest).at[tuple(beside)].set(top_value)


def shard_levels(stream_key, dims, shards, low, top_value):
    factor_of = 1.0
    for dim, shards_of in shards:
        draws = jax.random.uniform(jax.random.fold_in(jax.random.fold_in(stream_key, 6), dim), (shards_of,), jnp.float32, low / len(shards), top_value / len(shards))
        factor_of = factor_of * jnp.repeat(jnp.exp(draws), dims[dim] // shards_of).reshape((-1,) + (1,) * (len(dims) - 1 - dim))
    return factor_of


def gaussian(stream_key, shape, scale, reach, cuts=(), kind=jnp.bfloat16):
    values = scale * jax.random.normal(stream_key, shape, jnp.float32)
    if cuts:
        values = values * shard_levels(stream_key, shape, cuts, -0.22, 0.18)
    return jnp.clip(values, -reach, reach).astype(kind)


def setup_inputs(seed: int = 0) -> dict:
    arg_keys = jax.random.split(jax.random.key(seed), 12)
    normal_wind = gaussian(arg_keys[0], (BLOCKS, LEVELS, EDGES_DEV), 1.0, 6.0, ((0, 32),), jnp.float32)
    density = jnp.clip(0.5 + 1.0 * jax.random.uniform(arg_keys[1], (BLOCKS, LEVELS, CELLS_DEV), jnp.float32) ** shard_levels(arg_keys[1], (BLOCKS, LEVELS, CELLS_DEV), ((0, 32),), -0.2, 0.2), 0.5, 1.5)
    theta_field = gaussian(arg_keys[2], (BLOCKS, LEVELS, CELLS_DEV), 1.0, 6.0, ((0, 32),), jnp.float32)
    cell_edges = draw_cell_edges(jax.random.fold_in(arg_keys[11], 71), 0)
    edge_cells = draw_edge_cells(jax.random.fold_in(arg_keys[11], 71), 0)
    edges_on_edge = draw_edges_on_edge(jax.random.fold_in(arg_keys[11], 71), 0)
    send_cells = touch_ends(jax.random.randint(arg_keys[6], (BLOCKS, SLOTS, HALO_CELLS), 0, CELLS_DEV), jax.random.fold_in(arg_keys[6], 1), 0, CELLS_DEV - 1).astype(jnp.int32)
    send_edges = touch_ends(jax.random.randint(arg_keys[7], (BLOCKS, SLOTS, HALO_EDGES), 0, EDGES_DEV), jax.random.fold_in(arg_keys[7], 1), 0, EDGES_DEV - 1).astype(jnp.int32)
    cell_weight = gaussian(arg_keys[8], (BLOCKS, CELL_SIDES, CELLS_DEV), 1.0, 4.0, ((0, 32),), jnp.float32)
    eoe_weight = gaussian(arg_keys[9], (BLOCKS, EDGE_NEIGHBOURS, EDGES_DEV), EDGE_NEIGHBOURS ** -0.5, 2.0, ((0, 32),), jnp.float32)
    vert_coupling = jnp.clip(jnp.exp(math.log(4.0) - 4.3820266 * jax.random.uniform(arg_keys[10], (BLOCKS, LEVELS - 1, CELLS_DEV), jnp.float32) ** shard_levels(arg_keys[10], (BLOCKS, LEVELS - 1, CELLS_DEV), ((0, 32),), -0.2, 0.2)), 0.05, 4.0)
    return dict(normal_wind=normal_wind, density=density, theta_field=theta_field, cell_edges=cell_edges, edge_cells=edge_cells, edges_on_edge=edges_on_edge, send_cells=send_cells, send_edges=send_edges, cell_weight=cell_weight, eoe_weight=eoe_weight, vert_coupling=vert_coupling)


STEP_SIZE = 0.2
OFFSETS = (1, -1, 2, -2, 3, -3)


def column_solve(coupling, right_side):
    levels = right_side.shape[0]
    zero_row = jnp.zeros_like(right_side[0])
    ratios = []
    values = []
    ratio_prev = zero_row
    value_prev = zero_row
    for level_index in range(levels):
        coupling_below = coupling[level_index - 1] if level_index > 0 else zero_row
        coupling_above = coupling[level_index] if level_index < levels - 1 else zero_row
        divisor = 1.0 + coupling_below + coupling_above - coupling_below * ratio_prev
        ratio_now = coupling_above / divisor
        value_now = (right_side[level_index] + coupling_below * value_prev) / divisor
        ratios.append(ratio_now)
        values.append(value_now)
        ratio_prev = ratio_now
        value_prev = value_now
    result = [values[levels - 1]]
    for level_index in range(levels - 2, -1, -1):
        result.append(values[level_index] + ratios[level_index] * result[-1])
    return jnp.stack(result[::-1], axis=0)


def section_terms(density_ext, theta_ext, wind_ext, cell_edges, edge_cells, edges_on_edge, cell_weight, eoe_weight, coupling):
    owned_cells = cell_weight.shape[1]
    owned_edges = eoe_weight.shape[1]
    heat = density_ext * theta_ext
    both_ext = jnp.stack([density_ext, heat], axis=0)
    first_side = jnp.take(both_ext, edge_cells[0], axis=2)
    second_side = jnp.take(both_ext, edge_cells[1], axis=2)
    fluxes = wind_ext[None] * (0.5 * (first_side + second_side))
    density_tend = jnp.zeros((wind_ext.shape[0], owned_cells), jnp.float32)
    heat_sum = jnp.zeros((wind_ext.shape[0], owned_cells), jnp.float32)
    for side_index in range(cell_edges.shape[0]):
        weights = cell_weight[side_index]
        picked = jnp.take(fluxes, cell_edges[side_index], axis=2)
        density_tend = density_tend - weights * picked[0]
        heat_sum = heat_sum + weights * picked[1]
    theta_star = theta_ext[:, :owned_cells] - STEP_SIZE * heat_sum
    theta_new = column_solve(coupling, theta_star)
    tangential = jnp.zeros((wind_ext.shape[0], owned_edges), jnp.float32)
    for neighbour_index in range(edges_on_edge.shape[0]):
        tangential = tangential + eoe_weight[neighbour_index] * jnp.take(wind_ext, edges_on_edge[neighbour_index], axis=1)
    return density_tend, theta_new, tangential


def sender_of(block_index, slot_index):
    position = block_index // N_SUB
    side_index = block_index % N_SUB
    if slot_index < 6:
        return ((position - OFFSETS[slot_index]) % N_BLK) * N_SUB + side_index
    return position * N_SUB + (1 - side_index)


def select_block(stacked, block_index):
    return lax.dynamic_index_in_dim(stacked, block_index, 0, keepdims=False)


def extended(field, sends, block_index):
    pieces = [select_block(field, block_index)]
    for slot_index in range(7):
        source = sender_of(block_index, slot_index)
        send_rows = select_block(sends, source)[slot_index]
        source_field = select_block(field, source)
        pieces.append(jnp.take(source_field, send_rows, axis=1))
    return jnp.concatenate(pieces, axis=1)


def reference(normal_wind, density, theta_field, cell_edges, edge_cells, edges_on_edge, send_cells, send_edges, cell_weight, eoe_weight, vert_coupling):
    def one_block(block_index):
        density_ext = extended(density, send_cells, block_index)
        theta_ext = extended(theta_field, send_cells, block_index)
        wind_ext = extended(normal_wind, send_edges, block_index)
        return section_terms(density_ext, theta_ext, wind_ext, select_block(cell_edges, block_index), select_block(edge_cells, block_index), select_block(edges_on_edge, block_index), select_block(cell_weight, block_index), select_block(eoe_weight, block_index), select_block(vert_coupling, block_index))

    density_tend, theta_new, tangential = lax.map(one_block, jnp.arange(BLOCKS, dtype=jnp.int32))
    return (density_tend, theta_new, tangential)
```

```python
import jax
import jax.numpy as jnp
from jax import lax
from jax.experimental import pallas as pl
from jax.experimental.pallas import tpu as pltpu
from jax.sharding import PartitionSpec as P

STEP_SIZE = 0.2
OFFSETS = (1, -1, 2, -2, 3, -3)
F32 = jnp.float32
BF16 = jnp.bfloat16
ROWS = 64
PIECE = 64
CHUNK = 256
LANES = 128


def passed_along(block, axis, distance):
    devices = range(lax.axis_size(axis))
    route = [((i - distance) % len(devices), i) for i in devices]
    return lax.ppermute(block, axis, route)


def partner(value, axis, stride):
    mask = 2**stride
    pairs = [(source, source ^ mask) for source in range(lax.axis_size(axis))]
    return lax.ppermute(value, axis, pairs)


def halves(values):
    high = values.astype(BF16)
    low = (values - high.astype(F32)).astype(BF16)
    return high, low


def put_halves(ref, row, columns, values):
    high, low = halves(values)
    count = values.shape[0]
    ref[pl.ds(row, count), columns] = high
    ref[pl.ds(row + ROWS, count), columns] = low


def picks(base, count, indices, weights):
    pieces = []
    width = indices[0].shape[1]
    for start in range(0, count, PIECE):
        size = min(PIECE, count - start)
        rows = lax.broadcasted_iota(jnp.int32, (size, width), 0) + (base + start)
        matrix = jnp.zeros((size, width), F32)
        for index_row, weight_row in zip(indices, weights):
            matrix = jnp.where(rows == index_row, weight_row, matrix)
        pieces.append(matrix)
    return pieces


def exact_picks(base, count, indices, weights):
    return jnp.concatenate([p.astype(BF16) for p in picks(base, count, indices, weights)], axis=0)


def split_picks(base, count, indices, weights):
    pairs = [halves(p) for p in picks(base, count, indices, weights)]
    return (
        jnp.concatenate([p[0] for p in pairs], axis=0),
        jnp.concatenate([p[1] for p in pairs], axis=0),
    )


def mm(a, b):
    return jnp.dot(a, b, preferred_element_type=F32)


def merged_weights(indices, weights):
    merged = []
    for k, index_row in enumerate(indices):
        total = weights[k]
        for j in range(k):
            total = total + jnp.where(indices[j] == index_row, weights[j], 0.0)
        merged.append(total)
    return merged


def rows_of(ref, columns):
    return [ref[k : k + 1, columns] for k in range(ref.shape[0])]


def send_kernel(density, theta, wind, send_cells, send_edges, *rest):
    outs, (cells_split, wind_split) = rest[:-2], rest[-2:]
    levels = density.shape[0]
    every = slice(None)
    put_halves(cells_split, 0, every, density[...])
    put_halves(cells_split, 2 * ROWS, every, theta[...])
    put_halves(wind_split, 0, every, wind[...])
    one = jnp.ones((1, LANES), F32)
    for slot, out in enumerate(outs):
        cell_row = send_cells[slot : slot + 1, :]
        half = cell_row.shape[1]
        both = jnp.concatenate([cell_row, cell_row], axis=1)
        picked = mm(cells_split[...], exact_picks(0, density.shape[1], [both], [one]))
        lane = lax.broadcasted_iota(jnp.int32, (levels, 2 * half), 1)
        density_part = picked[0:levels] + picked[ROWS : ROWS + levels]
        theta_part = picked[2 * ROWS : 2 * ROWS + levels] + picked[3 * ROWS : 3 * ROWS + levels]
        out[:, 0 : 2 * half] = jnp.where(lane < half, density_part, theta_part)
        edge_row = send_edges[slot : slot + 1, :]
        picked = mm(wind_split[...], exact_picks(0, wind.shape[1], [edge_row], [one]))
        out[:, 2 * half :] = picked[0:levels] + picked[ROWS : ROWS + levels]


def pair_weights(first, second):
    return [jnp.full(first.shape, 0.5, F32), jnp.where(first == second, 1.0, 0.5)]


def tile(step):
    return pl.ds(pl.multiple_of(step * LANES, LANES), LANES)


def own_kernel(
    density, theta, wind, edge_cells, edges_on_edge, eoe_weight, cell_edges, cell_weight, coupling,
    average_own, tangent_own, eoe_merged, cell_merged, inverse, ratio, carry, cells_split, wind_split,
):
    levels, cells = density.shape
    edges = wind.shape[1]
    every = slice(None)
    put_halves(cells_split, 0, every, density[...])
    put_halves(cells_split, 2 * ROWS, every, density[...] * theta[...])
    put_halves(wind_split, 0, every, wind[...])
    for k, row in enumerate(merged_weights(rows_of(cell_edges, every), rows_of(cell_weight, every))):
        cell_merged[k : k + 1, :] = row
    ratio_prev = jnp.zeros((1, cells), F32)
    below = ratio_prev
    for level in range(levels):
        above = coupling[level : level + 1, :] if level < levels - 1 else jnp.zeros((1, cells), F32)
        inv = 1.0 / (1.0 + below + above - below * ratio_prev)
        ratio_prev = above * inv
        inverse[level : level + 1, :] = inv
        ratio[level : level + 1, :] = ratio_prev
        carry[level : level + 1, :] = below * inv
        below = above

    def average_step(step, _):
        columns = tile(step)
        pair = [edge_cells[0:1, columns], edge_cells[1:2, columns]]
        picked = mm(cells_split[...], exact_picks(0, cells, pair, pair_weights(*pair)))
        average_own[0:ROWS, columns] = picked[0:ROWS] + picked[ROWS : 2 * ROWS]
        average_own[ROWS : 2 * ROWS, columns] = picked[2 * ROWS : 3 * ROWS] + picked[3 * ROWS :]
        return 0

    lax.fori_loop(0, average_own.shape[1] // LANES, average_step, 0)

    def tangent_step(step, _):
        columns = tile(step)
        indices = rows_of(edges_on_edge, columns)
        weights = merged_weights(indices, rows_of(eoe_weight, columns))
        for k, row in enumerate(weights):
            eoe_merged[k : k + 1, columns] = row
        total = jnp.zeros((ROWS, LANES), F32)
        for start in range(0, edges, CHUNK):
            high, low = split_picks(start, CHUNK, indices, weights)
            picked = mm(wind_split[:, start : start + CHUNK], high)
            total = total + picked[0:ROWS] + picked[ROWS:]
            total = total + mm(wind_split[0:ROWS, start : start + CHUNK], low)
        tangent_own[:, columns] = total
        return 0

    lax.fori_loop(0, edges // LANES, tangent_step, 0)


def halo_kernel(
    *refs,
):
    received = refs[:7]
    (
        wind, theta, edge_cells, edges_on_edge, eoe_weight, cell_edges, cell_weight,
        average_own, tangent_own, inverse, ratio, carry,
        density_tend, theta_new, tangential,
        cells_split, wind_ext, wind_split, flux_split,
    ) = refs[7:]
    levels, cells = theta.shape
    edges = wind.shape[1]
    half = LANES // 2
    all_edges = edge_cells.shape[1]
    lane = lax.broadcasted_iota(jnp.int32, (levels, LANES), 1)
    wind_ext[0:levels, 0:edges] = wind[...]
    for first in range(0, 7, 2):
        here = received[first][:, 0:LANES]
        if first + 1 < 7:
            after = received[first + 1][:, 0:LANES]
        else:
            after = jnp.zeros_like(here)
        density_pair = jnp.where(lane < half, here, pltpu.roll(after, half, 1))
        theta_pair = jnp.where(lane < half, pltpu.roll(here, half, 1), after)
        columns = slice(first * half, first * half + LANES)
        put_halves(cells_split, 0, columns, density_pair)
        put_halves(cells_split, 2 * ROWS, columns, density_pair * theta_pair)
    for slot in range(7):
        values = received[slot][:, LANES:]
        start = edges + slot * LANES
        wind_ext[0:levels, start : start + LANES] = values
        put_halves(wind_split, 0, slice(slot * LANES, (slot + 1) * LANES), values)
    wind_split[:, 7 * LANES : 8 * LANES] = jnp.zeros((2 * ROWS, LANES), BF16)
    flux_split[:, all_edges:] = jnp.zeros((4 * ROWS, flux_split.shape[1] - all_edges), BF16)

    def flux_step(step, _):
        columns = tile(step)
        pair = [edge_cells[0:1, columns], edge_cells[1:2, columns]]
        picked = mm(cells_split[...], exact_picks(cells, 8 * half, pair, pair_weights(*pair)))
        wind_here = wind_ext[:, columns]
        average = average_own[0:ROWS, columns] + picked[0:ROWS] + picked[ROWS : 2 * ROWS]
        put_halves(flux_split, 0, columns, wind_here * average)
        average = average_own[ROWS : 2 * ROWS, columns] + picked[2 * ROWS : 3 * ROWS] + picked[3 * ROWS :]
        put_halves(flux_split, 2 * ROWS, columns, wind_here * average)
        return 0

    lax.fori_loop(0, all_edges // LANES, flux_step, 0)

    def tangent_step(step, _):
        columns = tile(step)
        indices = rows_of(edges_on_edge, columns)
        weights = rows_of(eoe_weight, columns)
        total = tangent_own[:, columns]
        for start in range(0, 8 * LANES, CHUNK):
            high, low = split_picks(edges + start, CHUNK, indices, weights)
            picked = mm(wind_split[:, start : start + CHUNK], high)
            total = total + picked[0:ROWS] + picked[ROWS:]
            total = total + mm(wind_split[0:ROWS, start : start + CHUNK], low)
        tangential[:, columns] = total[0:levels]
        return 0

    lax.fori_loop(0, edges // LANES, tangent_step, 0)

    for column in range(0, cells, LANES):
        columns = slice(column, column + LANES)
        indices = rows_of(cell_edges, columns)
        weights = rows_of(cell_weight, columns)

        def cell_step(step, total):
            start = pl.multiple_of(step * CHUNK, CHUNK)
            high, low = split_picks(start, CHUNK, indices, weights)
            values = flux_split[:, pl.ds(start, CHUNK)]
            picked = mm(values, high)
            extra = jnp.concatenate([values[0:ROWS], values[2 * ROWS : 3 * ROWS]], axis=0)
            return total + jnp.concatenate(
                [picked[0:ROWS] + picked[ROWS : 2 * ROWS], picked[2 * ROWS : 3 * ROWS] + picked[3 * ROWS :]], axis=0
            ) + mm(extra, low)

        total = lax.fori_loop(0, flux_split.shape[1] // CHUNK, cell_step, jnp.zeros((2 * ROWS, LANES), F32))
        density_tend[:, columns] = -total[0:levels]
        theta_new[:, columns] = (
            theta[:, columns] - STEP_SIZE * total[ROWS : ROWS + levels]
        ) * inverse[:, columns]
    value = theta_new[0:1, :]
    for level in range(1, levels):
        value = theta_new[level : level + 1, :] + carry[level : level + 1, :] * value
        theta_new[level : level + 1, :] = value
    for level in range(levels - 2, -1, -1):
        value = theta_new[level : level + 1, :] + ratio[level : level + 1, :] * value
        theta_new[level : level + 1, :] = value


def shape(*dims):
    return jax.ShapeDtypeStruct(dims, F32)


def shards(
    normal_wind,
    density,
    theta_field,
    cell_edges,
    edge_cells,
    edges_on_edge,
    send_cells,
    send_edges,
    cell_weight,
    eoe_weight,
    vert_coupling,
):
    wind_own = normal_wind[0]
    density_own = density[0]
    theta_own = theta_field[0]
    levels, cells = density_own.shape
    edges = wind_own.shape[1]
    slots, halo_cells = send_cells.shape[1:]
    halo_edges = send_edges.shape[2]
    all_edges = edge_cells.shape[2]
    vmem = pltpu.VMEM
    packed = pl.pallas_call(
        send_kernel,
        out_shape=[shape(levels, 2 * halo_cells + halo_edges)] * slots,
        scratch_shapes=[vmem((4 * ROWS, cells), BF16), vmem((2 * ROWS, edges), BF16)],
        name="send",
    )(density_own, theta_own, wind_own, send_cells[0], send_edges[0])
    received = [passed_along(packed[slot], "blk", OFFSETS[slot]) for slot in range(6)]
    received.append(partner(packed[6], "sub", 0))
    average_own, tangent_own, eoe_merged, cell_merged, inverse, ratio, carry = pl.pallas_call(
        own_kernel,
        out_shape=[
            shape(2 * ROWS, all_edges),
            shape(ROWS, edges),
            shape(*eoe_weight.shape[1:]),
            shape(*cell_weight.shape[1:]),
            shape(levels, cells),
            shape(levels, cells),
            shape(levels, cells),
        ],
        scratch_shapes=[vmem((4 * ROWS, cells), BF16), vmem((2 * ROWS, edges), BF16)],
        name="own",
    )(
        density_own, theta_own, wind_own, edge_cells[0], edges_on_edge[0], eoe_weight[0],
        cell_edges[0], cell_weight[0], vert_coupling[0],
    )
    density_tend, theta_new, tangential = pl.pallas_call(
        halo_kernel,
        out_shape=[shape(levels, cells), shape(levels, cells), shape(levels, edges)],
        scratch_shapes=[
            vmem((4 * ROWS, 8 * halo_cells), BF16),
            vmem((ROWS, all_edges), F32),
            vmem((2 * ROWS, 8 * halo_edges), BF16),
            vmem((4 * ROWS, -(-all_edges // CHUNK) * CHUNK), BF16),
        ],
        name="halo",
    )(
        *received, wind_own, theta_own, edge_cells[0], edges_on_edge[0], eoe_merged,
        cell_edges[0], cell_merged, average_own, tangent_own, inverse, ratio, carry,
    )
    return (density_tend[None], theta_new[None], tangential[None])


def solution(mesh):
    placed = P(("blk", "sub"), None, None)
    return jax.shard_map(
        shards,
        mesh=mesh,
        in_specs=(placed,) * 11,
        out_specs=(placed,) * 3,
        check_vma=False,
    )
```

```python
import jax
import jax.numpy as jnp
from jax import lax
from jax.experimental import pallas as pl
from jax.experimental.pallas import tpu as pltpu
from jax.sharding import PartitionSpec as P

STEP_SIZE = 0.2
OFFSETS = (1, -1, 2, -2, 3, -3)
F32 = jnp.float32
BF16 = jnp.bfloat16
ROWS = 64
PIECE = 32
CHUNK = 256
LANES = 128
UNROLL = True


def passed_along(block, axis, distance):
    devices = range(lax.axis_size(axis))
    route = [((i - distance) % len(devices), i) for i in devices]
    return lax.ppermute(block, axis, route)


def partner(value, axis, stride):
    mask = 2**stride
    pairs = [(source, source ^ mask) for source in range(lax.axis_size(axis))]
    return lax.ppermute(value, axis, pairs)


def halves(values):
    high = values.astype(BF16)
    low = (values - high.astype(F32)).astype(BF16)
    return high, low


def put_halves(ref, row, columns, values):
    high, low = halves(values)
    count = values.shape[0]
    ref[pl.ds(row, count), columns] = high
    ref[pl.ds(row + ROWS, count), columns] = low


def picks(base, count, indices, weights):
    pieces = []
    width = indices[0].shape[1]
    for start in range(0, count, PIECE):
        size = min(PIECE, count - start)
        rows = lax.broadcasted_iota(jnp.int32, (size, width), 0) + (base + start)
        matrix = jnp.zeros((size, width), F32)
        for index_row, weight_row in zip(indices, weights):
            matrix = jnp.where(rows == index_row, weight_row, matrix)
        pieces.append(matrix)
    return pieces


def exact_picks(base, count, indices, weights):
    return jnp.concatenate([p.astype(BF16) for p in picks(base, count, indices, weights)], axis=0)


def split_picks(base, count, indices, weights):
    pairs = [halves(p) for p in picks(base, count, indices, weights)]
    return (
        jnp.concatenate([p[0] for p in pairs], axis=0),
        jnp.concatenate([p[1] for p in pairs], axis=0),
    )


def mm(a, b):
    return jnp.dot(a, b, preferred_element_type=F32)


def merged_weights(indices, weights):
    merged = []
    for k, index_row in enumerate(indices):
        total = weights[k]
        for j in range(k):
            total = total + jnp.where(indices[j] == index_row, weights[j], 0.0)
        merged.append(total)
    return merged


def rows_of(ref, columns):
    return [ref[k, :, columns] for k in range(ref.shape[0])]


def flatten_rows(target, source):
    for level in range(source.shape[0]):
        target[level : level + 1, :] = source[level]


def send_kernel(density_rows, theta_rows, wind_rows, send_cells, send_edges, *rest):
    outs, (density, theta, wind, cells_split, wind_split) = rest[:-5], rest[-5:]
    levels = density.shape[0]
    every = slice(None)
    flatten_rows(density, density_rows)
    flatten_rows(theta, theta_rows)
    flatten_rows(wind, wind_rows)
    put_halves(cells_split, 0, every, density[...])
    put_halves(cells_split, 2 * ROWS, every, theta[...])
    put_halves(wind_split, 0, every, wind[...])
    one = jnp.ones((1, LANES), F32)
    for slot, out in enumerate(outs):
        cell_row = send_cells[slot]
        half = cell_row.shape[1]
        both = jnp.concatenate([cell_row, cell_row], axis=1)
        picked = mm(cells_split[...], exact_picks(0, density.shape[1], [both], [one]))
        lane = lax.broadcasted_iota(jnp.int32, (levels, 2 * half), 1)
        density_part = picked[0:levels] + picked[ROWS : ROWS + levels]
        theta_part = picked[2 * ROWS : 2 * ROWS + levels] + picked[3 * ROWS : 3 * ROWS + levels]
        out[:, 0 : 2 * half] = jnp.where(lane < half, density_part, theta_part)
        edge_row = send_edges[slot]
        picked = mm(wind_split[...], exact_picks(0, wind.shape[1], [edge_row], [one]))
        out[:, 2 * half :] = picked[0:levels] + picked[ROWS : ROWS + levels]


def pair_weights(first, second):
    return [jnp.full(first.shape, 0.5, F32), jnp.where(first == second, 1.0, 0.5)]


def tile(step, width=LANES):
    return pl.ds(pl.multiple_of(step * width, width), width)


def own_kernel(
    density, theta, wind, edge_cells, edges_on_edge, eoe_weight, cell_edges, cell_weight, coupling,
    average_own, tangent_own, eoe_merged, cell_merged, inverse, ratio, carry, cells_split, wind_split,
):
    levels, cells = density.shape
    edges = wind.shape[1]
    every = slice(None)
    put_halves(cells_split, 0, every, density[...])
    put_halves(cells_split, 2 * ROWS, every, density[...] * theta[...])
    put_halves(wind_split, 0, every, wind[...])
    for k, row in enumerate(merged_weights(rows_of(cell_edges, every), rows_of(cell_weight, every))):
        cell_merged[k] = row
    ratio_prev = jnp.zeros((1, cells), F32)
    below = ratio_prev
    for level in range(levels):
        above = coupling[level] if level < levels - 1 else jnp.zeros((1, cells), F32)
        inv = 1.0 / (1.0 + below + above - below * ratio_prev)
        ratio_prev = above * inv
        inverse[level : level + 1, :] = inv
        ratio[level : level + 1, :] = ratio_prev
        carry[level : level + 1, :] = below * inv
        below = above

    def average_step(step, _):
        columns = tile(step)
        pair = [edge_cells[0:1, columns], edge_cells[1:2, columns]]
        picked = mm(cells_split[...], exact_picks(0, cells, pair, pair_weights(*pair)))
        average_own[0:ROWS, columns] = picked[0:ROWS] + picked[ROWS : 2 * ROWS]
        average_own[ROWS : 2 * ROWS, columns] = picked[2 * ROWS : 3 * ROWS] + picked[3 * ROWS :]
        return 0

    lax.fori_loop(0, average_own.shape[1] // LANES, average_step, 0, unroll=UNROLL)

    width = CHUNK if edges % CHUNK == 0 else LANES

    def tangent_step(step, _):
        columns = tile(step, width)
        indices = rows_of(edges_on_edge, columns)
        weights = merged_weights(indices, rows_of(eoe_weight, columns))
        for k, row in enumerate(weights):
            eoe_merged[k, :, columns] = row
        total = jnp.zeros((ROWS, width), F32)
        for start in range(0, edges, CHUNK):
            high, low = split_picks(start, CHUNK, indices, weights)
            picked = mm(wind_split[:, start : start + CHUNK], high)
            total = total + picked[0:ROWS] + picked[ROWS:]
            total = total + mm(wind_split[0:ROWS, start : start + CHUNK], low)
        tangent_own[:, columns] = total
        return 0

    lax.fori_loop(0, edges // width, tangent_step, 0, unroll=UNROLL)


def halo_kernel(
    *refs,
):
    received = refs[:7]
    (
        wind, theta, edge_cells, edges_on_edge, eoe_weight, cell_edges, cell_weight,
        average_own, tangent_own, inverse, ratio, carry,
        density_tend, theta_new, tangential,
        cells_split, wind_ext, wind_split, flux_split, tangent_sum, solved,
    ) = refs[7:]
    levels, cells = theta.shape
    edges = wind.shape[1]
    half = LANES // 2
    all_edges = edge_cells.shape[1]
    lane = lax.broadcasted_iota(jnp.int32, (levels, LANES), 1)
    wind_ext[0:levels, 0:edges] = wind[...]
    for first in range(0, 7, 2):
        here = received[first][:, 0:LANES]
        if first + 1 < 7:
            after = received[first + 1][:, 0:LANES]
        else:
            after = jnp.zeros_like(here)
        density_pair = jnp.where(lane < half, here, pltpu.roll(after, half, 1))
        theta_pair = jnp.where(lane < half, pltpu.roll(here, half, 1), after)
        columns = slice(first * half, first * half + LANES)
        put_halves(cells_split, 0, columns, density_pair)
        put_halves(cells_split, 2 * ROWS, columns, density_pair * theta_pair)
    for slot in range(7):
        values = received[slot][:, LANES:]
        start = edges + slot * LANES
        wind_ext[0:levels, start : start + LANES] = values
        put_halves(wind_split, 0, slice(slot * LANES, (slot + 1) * LANES), values)
    wind_split[:, 7 * LANES : 8 * LANES] = jnp.zeros((2 * ROWS, LANES), BF16)
    flux_split[:, all_edges:] = jnp.zeros((4 * ROWS, flux_split.shape[1] - all_edges), BF16)

    def flux_step(step, _):
        columns = tile(step)
        pair = [edge_cells[0:1, columns], edge_cells[1:2, columns]]
        picked = mm(cells_split[...], exact_picks(cells, 8 * half, pair, pair_weights(*pair)))
        wind_here = wind_ext[:, columns]
        average = average_own[0:ROWS, columns] + picked[0:ROWS] + picked[ROWS : 2 * ROWS]
        put_halves(flux_split, 0, columns, wind_here * average)
        average = average_own[ROWS : 2 * ROWS, columns] + picked[2 * ROWS : 3 * ROWS] + picked[3 * ROWS :]
        put_halves(flux_split, 2 * ROWS, columns, wind_here * average)
        return 0

    lax.fori_loop(0, all_edges // LANES, flux_step, 0, unroll=UNROLL)

    width = CHUNK if edges % CHUNK == 0 else LANES

    def tangent_step(step, _):
        columns = tile(step, width)
        indices = rows_of(edges_on_edge, columns)
        weights = rows_of(eoe_weight, columns)
        total = tangent_own[:, columns]
        for start in range(0, 8 * LANES, CHUNK):
            high, low = split_picks(edges + start, CHUNK, indices, weights)
            picked = mm(wind_split[:, start : start + CHUNK], high)
            total = total + picked[0:ROWS] + picked[ROWS:]
            total = total + mm(wind_split[0:ROWS, start : start + CHUNK], low)
        tangent_sum[:, columns] = total
        return 0

    lax.fori_loop(0, edges // width, tangent_step, 0, unroll=UNROLL)

    for level in range(levels):
        tangential[level] = tangent_sum[level : level + 1, :]
    width = CHUNK if cells % CHUNK == 0 else LANES
    for column in range(0, cells, width):
        columns = slice(column, column + width)
        indices = rows_of(cell_edges, columns)
        weights = rows_of(cell_weight, columns)

        def cell_step(step, total):
            start = pl.multiple_of(step * CHUNK, CHUNK)
            high, low = split_picks(start, CHUNK, indices, weights)
            values = flux_split[:, pl.ds(start, CHUNK)]
            picked = mm(values, high)
            extra = jnp.concatenate([values[0:ROWS], values[2 * ROWS : 3 * ROWS]], axis=0)
            return total + jnp.concatenate(
                [picked[0:ROWS] + picked[ROWS : 2 * ROWS], picked[2 * ROWS : 3 * ROWS] + picked[3 * ROWS :]], axis=0
            ) + mm(extra, low)

        total = lax.fori_loop(0, flux_split.shape[1] // CHUNK, cell_step, jnp.zeros((2 * ROWS, width), F32), unroll=UNROLL)
        for level in range(levels):
            density_tend[level, :, columns] = -total[level : level + 1]
        solved[:, columns] = (
            theta[:, columns] - STEP_SIZE * total[ROWS : ROWS + levels]
        ) * inverse[:, columns]
    value = solved[0:1, :]
    for level in range(1, levels):
        value = solved[level : level + 1, :] + carry[level : level + 1, :] * value
        solved[level : level + 1, :] = value
    theta_new[levels - 1] = value
    for level in range(levels - 2, -1, -1):
        value = solved[level : level + 1, :] + ratio[level : level + 1, :] * value
        theta_new[level] = value


def rowwise(values):
    return jnp.transpose(values, (1, 0, 2))


def shape(*dims):
    return jax.ShapeDtypeStruct(dims, F32)


def shards(
    normal_wind,
    density,
    theta_field,
    cell_edges,
    edge_cells,
    edges_on_edge,
    send_cells,
    send_edges,
    cell_weight,
    eoe_weight,
    vert_coupling,
):
    levels, cells = density.shape[1:]
    edges = normal_wind.shape[2]
    slots, halo_cells = send_cells.shape[1:]
    halo_edges = send_edges.shape[2]
    all_edges = edge_cells.shape[2]
    vmem = pltpu.VMEM
    packed = pl.pallas_call(
        send_kernel,
        out_shape=[shape(levels, 2 * halo_cells + halo_edges)] * slots
        + [shape(levels, cells), shape(levels, cells), shape(levels, edges)],
        scratch_shapes=[vmem((4 * ROWS, cells), BF16), vmem((2 * ROWS, edges), BF16)],
        name="send",
    )(rowwise(density), rowwise(theta_field), rowwise(normal_wind), rowwise(send_cells), rowwise(send_edges))
    density_own, theta_own, wind_own = packed[slots:]
    received = [passed_along(packed[slot], "blk", OFFSETS[slot]) for slot in range(6)]
    received.append(partner(packed[6], "sub", 0))
    average_own, tangent_own, eoe_merged, cell_merged, inverse, ratio, carry = pl.pallas_call(
        own_kernel,
        out_shape=[
            shape(2 * ROWS, all_edges),
            shape(ROWS, edges),
            shape(eoe_weight.shape[1], 1, edges),
            shape(cell_weight.shape[1], 1, cells),
            shape(levels, cells),
            shape(levels, cells),
            shape(levels, cells),
        ],
        scratch_shapes=[vmem((4 * ROWS, cells), BF16), vmem((2 * ROWS, edges), BF16)],
        name="own",
    )(
        density_own, theta_own, wind_own, edge_cells[0], rowwise(edges_on_edge), rowwise(eoe_weight),
        rowwise(cell_edges), rowwise(cell_weight), rowwise(vert_coupling),
    )
    density_tend, theta_new, tangential = pl.pallas_call(
        halo_kernel,
        out_shape=[shape(levels, 1, cells), shape(levels, 1, cells), shape(levels, 1, edges)],
        scratch_shapes=[
            vmem((4 * ROWS, 8 * halo_cells), BF16),
            vmem((ROWS, all_edges), F32),
            vmem((2 * ROWS, 8 * halo_edges), BF16),
            vmem((4 * ROWS, -(-all_edges // CHUNK) * CHUNK), BF16),
            vmem((ROWS, edges), F32),
            vmem((levels, cells), F32),
        ],
        name="halo",
    )(
        *received, wind_own, theta_own, edge_cells[0], rowwise(edges_on_edge), eoe_merged,
        rowwise(cell_edges), cell_merged, average_own, tangent_own, inverse, ratio, carry,
    )
    return (rowwise(density_tend), rowwise(theta_new), rowwise(tangential))


def solution(mesh):
    placed = P(("blk", "sub"), None, None)
    return jax.shard_map(
        shards,
        mesh=mesh,
        in_specs=(placed,) * 11,
        out_specs=(placed,) * 3,
        check_vma=False,
    )
```
